32 devices in a mesh: fac: 8 (over z, y), cust: 4 (over x, core).
Axes of the slice: x: 2, y: 2, z: 4, core: 2. Of those that a mesh axis runs over, the one named last changes fastest.
Arguments:
- fac_coords: bfloat16 [4096, 128], P('fac'), may hold values from -6 to 6
- cust_coords: bfloat16 [65536, 128], P(('cust', 'fac')), may hold values from -6 to 6
- open_flags: int32 [4096], P('fac'), may hold values 0 or 1
- demand: int32 [65536], P('cust'), may hold values from 1 to 4
- fixed_cost: float32 [4096], P('fac'), may hold values from 0 to 64
- capacity: float32 [4096], P('fac'), may hold values from 32 to 128
- cap_mult: float32 [4096], P('fac'), may hold values from 0 to 0.1
- cover_mult: float32 [65536], P('cust'), may hold values from 0 to 2, as said below
Outputs:
- cover_final: float32 [65536], P('cust')
- cap_final: float32 [4096], P('fac')
- bounds: float32 [3], replicated
The draws below stay inside these ranges and needn't reach their ends.
Inputs may be any that keep to these rules, and one draw needn't show every extreme that they name: `cover_mult`: initial coverage multipliers, all in one band of width 0.4.
All inputs are finite; a program needn't handle non-finite values. No bound on the sum of `open_flags` on one device may be relied on, other than what follows from the above.
Results may differ from the reference program's by a relative error of at most 0.0003.
Values may be sent and summed in bfloat16 or wider, within the bound.
A program may use at most 64 MiB of HBM per device.

```python
import math
import jax
import jax.numpy as jnp
from jax import lax

K = 128
ITERS = 3
F = 4096
C = 65536


def draw_cover_mult(key, part):
    tau = 0.1
    level = 2.125 - tau * (math.log(F / 2.0) + 300.0 / K)
    spread = jax.random.uniform(key, (C,), jnp.float32, -0.2, 0.2)
    return (level + spread).astype(jnp.float32)


def with_ends(array, rng, smallest, top_value):
    index_at = [jax.random.randint(jax.random.fold_in(rng, axis), (), 0, length) for axis, length in enumerate(array.shape)]
    longest = array.shape.index(max(array.shape))
    neighbour = index_at[:longest] + [(index_at[longest] + 1) % array.shape[longest]] + index_at[longest + 1:]
    return array.at[tuple(index_at)].set(smallest).at[tuple(neighbour)].set(top_value)


def levels(own_key, dims, split, low, high):
    def one(dim, blocks):
        heights = jax.random.uniform(jax.random.fold_in(jax.random.fold_in(own_key, 6), dim), (blocks,), jnp.float32, low / len(split), high / len(split))
        return jnp.repeat(jnp.exp(heights), dims[dim] // blocks).reshape((-1,) + (1,) * (len(dims) - dim - 1))

    loudness = one(*split[0])
    for cut in split[1:]:
        loudness = loudness * one(*cut)
    return loudness


def noise(stream_key, shape, scale, reach, pieces=(), kind=jnp.bfloat16):
    gain = levels(stream_key, shape, pieces, -0.22, 0.18) if pieces else 1.0
    entries = jax.random.normal(stream_key, shape, jnp.float32) * scale * gain
    return jnp.minimum(jnp.maximum(entries, -reach), reach).astype(kind)


def setup_inputs(seed: int = 0) -> dict:
    key_of = jax.random.split(jax.random.key(seed), 9)
    return {
        "fac_coords": noise(key_of[0], (F, K), 1.0, 6.0, ((0, 8),)),
        "cust_coords": noise(key_of[1], (C, K), 1.0, 6.0, ((0, 32),)),
        "open_flags": with_ends((jax.random.randint(key_of[2], (F,), 0, 2) < 1).astype(jnp.int32), jax.random.fold_in(key_of[2], 1), 0, 1),
        "demand": with_ends(jax.random.randint(key_of[3], (C,), 1, 5), jax.random.fold_in(key_of[3], 1), 1, 4).astype(jnp.int32),
        "fixed_cost": jnp.clip(64.0 * jax.random.uniform(key_of[4], (F,), jnp.float32) ** levels(key_of[4], (F,), ((0, 8),), -0.2, 0.2), 0.0, 64.0),
        "capacity": jnp.clip(32.0 + 96.0 * jax.random.uniform(key_of[5], (F,), jnp.float32) ** levels(key_of[5], (F,), ((0, 8),), -0.2, 0.2), 32.0, 128.0),
        "cap_mult": jnp.clip(0.1 * jax.random.uniform(key_of[6], (F,), jnp.float32) ** levels(key_of[6], (F,), ((0, 8),), -0.2, 0.2), 0.0, 0.1),
        "cover_mult": draw_cover_mult(jax.random.fold_in(key_of[8], 71), 0),
    }


def reference(fac_coords, cust_coords, open_flags, demand, fixed_cost, capacity, cap_mult, cover_mult):
    tau = 0.1
    fac_block = 256
    n_fac = fac_coords.shape[0]
    n_cust = cust_coords.shape[0]
    width = fac_coords.shape[1]
    fac_block = min(fac_block, n_fac)
    opened = open_flags.astype(jnp.float32)
    weight = demand.astype(jnp.float32)
    pnorm = jnp.sum(fac_coords.astype(jnp.float32) ** 2, axis=1)
    qnorm = jnp.sum(cust_coords.astype(jnp.float32) ** 2, axis=1)
    blocks = n_fac // fac_block
    lam = cover_mult
    mu = cap_mult
    bound_list = []
    for step in range(ITERS):
        size = 0.1 / (step + 1)

        def one_block(cover, index):
            start = (index * fac_block).astype(jnp.int32)
            rows = lax.dynamic_slice_in_dim(fac_coords, start, fac_block, 0)
            pn = lax.dynamic_slice_in_dim(pnorm, start, fac_block, 0)
            mu_b = lax.dynamic_slice_in_dim(mu, start, fac_block, 0)
            op_b = lax.dynamic_slice_in_dim(opened, start, fac_block, 0)
            dots = lax.dot_general(rows, cust_coords, (((1,), (1,)), ((), ())), preferred_element_type=jnp.float32)
            cost = (pn[:, None] + qnorm[None, :] - 2.0 * dots) / width
            zval = (lam[None, :] - cost - mu_b[:, None] * weight[None, :]) / tau
            share = op_b[:, None] * jax.nn.sigmoid(zval)
            load_b = jnp.sum(share * weight[None, :], axis=1)
            soft_b = -tau * op_b * jnp.sum(jax.nn.softplus(zval) * weight[None, :], axis=1)
            return cover + jnp.sum(share, axis=0), (load_b, soft_b)

        cover, pair = lax.scan(one_block, jnp.zeros((n_cust,), jnp.float32), jnp.arange(blocks, dtype=jnp.int32))
        load = pair[0].reshape(n_fac)
        soft = pair[1].reshape(n_fac)
        bound = (jnp.sum(weight * lam) + jnp.sum(opened * fixed_cost - mu * capacity + soft)) / n_cust
        bound_list.append(bound)
        lam = lam + size * weight * (1.0 - cover) / (1.0 + cover)
        mu = jnp.maximum(0.0, mu + size * (load - capacity) / (load + capacity))
    return lam, mu, jnp.stack(bound_list).astype(jnp.float32)
```

```python
import functools
import math

import jax
import jax.numpy as jnp
from jax import lax
from jax.experimental import pallas as pl
from jax.experimental.pallas import tpu as pltpu
from jax.sharding import PartitionSpec as P

MESH = pl.DeviceIdType.MESH
ITERS = 3
TAU = 0.1
ALIGN = 16
ROWS = 256
F32 = jnp.float32
BF16 = jnp.bfloat16
VMEM = pl.BlockSpec(memory_space=pltpu.VMEM)


def split3(v):
    a = v.astype(BF16)
    r = v - a.astype(F32)
    b = r.astype(BF16)
    c = (r - b.astype(F32)).astype(BF16)
    return a, b, c


def onehot_of(open_row):
    n = open_row.shape[1]
    flags = jnp.broadcast_to(open_row.astype(F32), (16, n)).astype(BF16)
    tri = (lax.broadcasted_iota(jnp.int32, (n, n), 0) <= lax.broadcasted_iota(jnp.int32, (n, n), 1)).astype(F32).astype(BF16)
    pos = jnp.dot(flags, tri, preferred_element_type=F32)[0:1]
    pos = jnp.where(open_row > 0, pos - 1.0, -1.0).astype(jnp.int32)
    hit = lax.broadcasted_iota(jnp.int32, (n, n), 0) == pos
    return jnp.where(hit, 1.0, 0.0).astype(BF16)


def nt(a, b):
    return lax.dot_general(a, b, (((1,), (1,)), ((), ())), preferred_element_type=F32)


def pre_kernel(open_ref, fac_ref, cap_ref, mu_ref, cust_ref, comp_ref, info_ref, cust_t_ref, hq_ref):
    n, width = fac_ref.shape
    hot = onehot_of(open_ref[...])
    fac = fac_ref[...]
    comp_ref[...] = jnp.dot(hot, fac, preferred_element_type=F32).astype(BF16)
    sq = fac.astype(F32) ** 2
    s1, s2, _ = split3(sq)
    ones = jnp.ones((16, width), BF16)
    half = -0.5 * (nt(ones, s1) + nt(ones, s2))[0:1]
    rows = [jnp.ones((1, n), BF16)]
    for v in (half, mu_ref[...], cap_ref[...]):
        rows.extend(split3(v))
    rows = [r.astype(F32) for r in rows] + [jnp.zeros((6, n), F32)]
    got = nt(jnp.concatenate(rows, axis=0).astype(BF16), hot)
    info_ref[0:1, :] = got[0:1]
    for m in range(3):
        info_ref[m + 1:m + 2, :] = got[3 * m + 1:3 * m + 2] + got[3 * m + 2:3 * m + 3] + got[3 * m + 3:3 * m + 4]
    info_ref[4:8, :] = jnp.zeros((4, n), F32)
    eye = (lax.broadcasted_iota(jnp.int32, (width, width), 0) == lax.broadcasted_iota(jnp.int32, (width, width), 1)).astype(F32).astype(BF16)
    turned = nt(eye, cust_ref[...])
    cust_t_ref[...] = turned.astype(BF16)
    hq_ref[...] = 0.5 * jnp.sum(turned * turned, axis=0, keepdims=True)


def sync(peers):
    barrier = pltpu.get_barrier_semaphore()
    for peer in peers:
        pl.semaphore_signal(barrier, inc=1, device_id=peer, device_id_type=MESH)
    pl.semaphore_wait(barrier, len(peers))


def gather_kernel(nf, nc, comp_ref, info_ref, facs_ref, infos_ref, s1, r1, s2, r2, s3, r3, loc):
    f, c = lax.axis_index("fac"), lax.axis_index("cust")
    fp = [(lax.rem(f + d, nf), c) for d in range(1, nf)]
    cp = [(f, lax.rem(c + d, nc)) for d in range(1, nc)]
    n = comp_ref.shape[0]
    part = n // nc
    sync(fp + cp)
    mine = pl.ds(pl.multiple_of(c * part, part), part)
    own = pltpu.make_async_copy(comp_ref, facs_ref.at[f], loc.at[0])
    own.start()
    own_info = pltpu.make_async_copy(info_ref, infos_ref.at[f], loc.at[1])
    own_info.start()
    sends = []
    for d, peer in enumerate(fp):
        cpy = pltpu.make_async_remote_copy(comp_ref.at[mine], facs_ref.at[f, mine], s1.at[d], r1.at[d], device_id=peer, device_id_type=MESH)
        cpy.start()
        sends.append(cpy)
        cpy = pltpu.make_async_remote_copy(info_ref, infos_ref.at[f], s3.at[d], r3.at[d], device_id=peer, device_id_type=MESH)
        cpy.start()
        sends.append(cpy)
    seconds = []
    for d in range(nf - 1):
        src = lax.rem(f + nf - 1 - d, nf)
        sends[2 * d].wait_recv()
        for e, peer in enumerate(cp):
            cpy = pltpu.make_async_remote_copy(facs_ref.at[src, mine], facs_ref.at[src, mine], s2.at[d, e], r2.at[d, e], device_id=peer, device_id_type=MESH)
            cpy.start()
            seconds.append(cpy)
    for d in range(nf - 1):
        sends[2 * d].wait_send()
        sends[2 * d + 1].wait()
    for cpy in seconds:
        cpy.wait()
    own.wait()
    own_info.wait()


def step_kernel(first, size, prev, facs_ref, info_ref, mu_ref, load_ref, cust_t_ref, hq_ref, lam_ref, wt_ref,
                part_ref, mu_out_ref, lam_out_ref, tot_ref,
                a_ref, w_ref, y_ref, acc_ref, cov_ref, soft_ref):
    nf, n, width = facs_ref.shape
    cols = cust_t_ref.shape[1]
    block = y_ref.shape[2]
    tiles = cols // block
    lam = lam_ref[...]
    wt = wt_ref[...]
    a1, a2, a3 = split3(64.0 * lam - hq_ref[...])
    one_c = jnp.ones((3, cols), F32)
    mw = jnp.broadcast_to(-64.0 * wt, (3, cols))
    aug = jnp.concatenate([a1.astype(F32), a2.astype(F32), a3.astype(F32), one_c, mw, jnp.zeros((7, cols), F32)], axis=0)
    w_ref[0:width, :] = cust_t_ref[...]
    w_ref[width:width + 16, :] = aug.astype(BF16)
    w_ref[width + 16:, :] = jnp.zeros((width - 16, cols), BF16)
    cov_ref[...] = jnp.zeros_like(cov_ref)
    soft_ref[...] = jnp.zeros_like(soft_ref)
    lane = lax.broadcasted_iota(jnp.int32, (ROWS, width), 1)
    pad = jnp.where(lane == 3, -30000.0, 0.0).astype(BF16)
    sel = (lax.broadcasted_iota(jnp.int32, (16, width), 0) == lax.broadcasted_iota(jnp.int32, (16, width), 1)).astype(F32).astype(BF16)
    offs = []
    off = jnp.int32(0)
    one_r = jnp.ones((3, n), F32)
    for f in range(nf):
        valid = info_ref[f, 0:1, :]
        cap = info_ref[f, 3:4, :]
        if first:
            mu = info_ref[f, 2:3, :]
        else:
            mu = mu_ref[f:f + 1, :]
            load = load_ref[f:f + 1, :]
            mu = jnp.maximum(0.0, mu + prev * (load - cap) / (load + jnp.where(valid > 0, cap, 1.0)))
        mu = mu * valid
        mu_out_ref[f:f + 1, :] = mu
        b = jnp.where(valid > 0, info_ref[f, 1:2, :], -30000.0)
        parts = [p.astype(F32) for p in split3(b) + split3(mu)]
        rows = jnp.concatenate([one_r] + parts + [jnp.zeros((7, n), F32)], axis=0).astype(BF16)
        side = lax.dot_general(rows, sel, (((0,), (0,)), ((), ())), preferred_element_type=F32).astype(BF16)
        count = jnp.sum(valid).astype(jnp.int32)
        off = pl.multiple_of(off, ALIGN)
        offs.append(off)
        a_ref[pl.ds(off, n), 0:width] = facs_ref[f]
        a_ref[pl.ds(off, n), width:2 * width] = side
        off = off + ((count + ALIGN - 1) // ALIGN) * ALIGN
    tail = pl.multiple_of(off, ALIGN)
    a_ref[pl.ds(tail, ROWS), 0:width] = jnp.zeros((ROWS, width), BF16)
    a_ref[pl.ds(tail, ROWS), width:2 * width] = pad
    n_blocks = (off + ROWS - 1) // ROWS
    scale = math.log2(math.e) / 6.4

    def body(i, _):
        base = pl.multiple_of(i * ROWS, ROWS)
        lhs = a_ref[pl.ds(base, ROWS), :]

        def dot(t):
            y_ref[t % 2] = jnp.dot(lhs, w_ref[:, t * block:(t + 1) * block], preferred_element_type=F32)

        dot(0)
        for t in range(tiles):
            if t + 1 < tiles:
                dot(t + 1)
            covs = [cov_ref[:, t * block + q * 128:t * block + (q + 1) * 128] for q in range(block // 128)]
            softs = [soft_ref[:, t * block + q * 128:t * block + (q + 1) * 128] for q in range(block // 128)]
            for r in range(0, ROWS, 32):
                loads = [None] * 4
                for q in range(block // 128):
                    at = t * block + q * 128
                    wq = jnp.broadcast_to(wt_ref[:, at:at + 128], (8, 128))
                    es = [jnp.exp2(y_ref[t % 2, r + 8 * s:r + 8 * s + 8, q * 128:(q + 1) * 128] * scale) for s in range(4)]
                    us = [1.0 + e for e in es]
                    p01 = us[0] * us[1]
                    p23 = us[2] * us[3]
                    r01 = 1.0 / p01
                    r23 = 1.0 / p23
                    xs = [es[0] * (us[1] * r01), es[1] * (us[0] * r01), es[2] * (us[3] * r23), es[3] * (us[2] * r23)]
                    covs[q] = covs[q] + ((xs[0] + xs[1]) + (xs[2] + xs[3]))
                    softs[q] = softs[q] + jnp.log(p01 * p23)
                    for s in range(4):
                        v = xs[s] * wq
                        loads[s] = v if loads[s] is None else loads[s] + v
                for s in range(4):
                    at = pl.ds(base + r + 8 * s, 8)
                    if t == 0:
                        acc_ref[at, :] = loads[s]
                    else:
                        acc_ref[at, :] = acc_ref[at, :] + loads[s]
            for q in range(block // 128):
                cov_ref[:, t * block + q * 128:t * block + (q + 1) * 128] = covs[q]
                soft_ref[:, t * block + q * 128:t * block + (q + 1) * 128] = softs[q]
        return 0

    lax.fori_loop(0, n_blocks, body, 0)
    ones = jnp.ones((8, 128), F32)
    for f in range(nf):
        got = lax.dot_general(ones, acc_ref[pl.ds(offs[f], n), :], (((1,), (1,)), ((), ())), preferred_element_type=F32, precision=lax.Precision.HIGHEST)
        part_ref[f:f + 1, :] = jnp.where(info_ref[f, 0:1, :] > 0, got[0:1], 0.0)
    cover = jnp.sum(cov_ref[...], axis=0, keepdims=True)
    soft = jnp.sum(soft_ref[...], axis=0, keepdims=True)
    tot_ref[...] = jnp.full((8, 128), jnp.sum(wt * lam - TAU * wt * soft), F32)
    lam_out_ref[...] = lam + size * wt * (1.0 - cover) / (1.0 + cover)


def exchange(peers, src, slots, send, recv):
    copies = []
    for d, peer in enumerate(peers):
        cpy = pltpu.make_async_remote_copy(src, slots.at[d], send.at[d], recv.at[d], device_id=peer, device_id_type=MESH)
        cpy.start()
        copies.append(cpy)
    return copies


def reduce_kernel(nf, nc, x_ref, out_ref, got1, mid, got2, s1, r1, s2, r2):
    f, c = lax.axis_index("fac"), lax.axis_index("cust")
    fp = [(lax.rem(f + d, nf), c) for d in range(1, nf)]
    cp = [(f, lax.rem(c + d, nc)) for d in range(1, nc)]
    sync(fp + cp)
    first = exchange(cp, x_ref, got1, s1, r1)
    total = x_ref[...]
    for d, cpy in enumerate(first):
        cpy.wait()
        total = total + got1[d]
    mid[...] = total
    second = exchange(fp, mid, got2, s2, r2)
    for d, cpy in enumerate(second):
        cpy.wait()
        total = total + got2[d]
    out_ref[...] = total


def gather_lam_kernel(nf, lam_ref, out_ref, s1, r1, loc):
    f, c = lax.axis_index("fac"), lax.axis_index("cust")
    fp = [(lax.rem(f + d, nf), c) for d in range(1, nf)]
    sync(fp)
    own = pltpu.make_async_copy(lam_ref, out_ref.at[f], loc)
    own.start()
    copies = []
    for d, peer in enumerate(fp):
        cpy = pltpu.make_async_remote_copy(lam_ref, out_ref.at[f], s1.at[d], r1.at[d], device_id=peer, device_id_type=MESH)
        cpy.start()
        copies.append(cpy)
    for cpy in copies:
        cpy.wait()
    own.wait()


def params(cid=None, mib=56):
    return pltpu.CompilerParams(collective_id=cid, has_side_effects=True, vmem_limit_bytes=mib * 2 ** 20) if cid is not None else pltpu.CompilerParams(vmem_limit_bytes=mib * 2 ** 20)


def local(nf, nc, fac_coords, cust_coords, open_flags, demand, fixed_cost, capacity, cap_mult, cover_mult):
    n, width = fac_coords.shape
    cols = cust_coords.shape[0]
    total_cust = cols * nf * nc
    f = lax.axis_index("fac")
    c = lax.axis_index("cust")
    sd = jax.ShapeDtypeStruct
    dma = pltpu.SemaphoreType.DMA
    wt = lax.dynamic_slice_in_dim(demand, f * cols, cols).astype(F32).reshape(1, cols)
    lam = lax.dynamic_slice_in_dim(cover_mult, f * cols, cols).reshape(1, cols)
    open_row = open_flags.reshape(1, n)
    comp, info, cust_t, hq = pl.pallas_call(
        pre_kernel,
        out_shape=(sd((n, width), BF16), sd((8, n), F32), sd((width, cols), BF16), sd((1, cols), F32)),
        in_specs=[VMEM] * 5, out_specs=(VMEM,) * 4, compiler_params=params(), name="pre",
    )(open_row, fac_coords, capacity.reshape(1, n), cap_mult.reshape(1, n), cust_coords)
    facs, infos = pl.pallas_call(
        functools.partial(gather_kernel, nf, nc),
        out_shape=(sd((nf, n, width), BF16), sd((nf, 8, n), F32)),
        in_specs=[VMEM] * 2, out_specs=(VMEM,) * 2,
        scratch_shapes=[dma((nf - 1,)), dma((nf - 1,)), dma((nf - 1, nc - 1)), dma((nf - 1, nc - 1)), dma((nf - 1,)), dma((nf - 1,)), dma((2,))],
        compiler_params=params(0), name="gather",
    )(comp, info)
    block = math.gcd(cols, 512)
    total_rows = nf * n
    tots = []
    mus = []
    mu = load = jnp.zeros((nf, n), F32)
    for step in range(ITERS):
        part, mu, lam, tot = pl.pallas_call(
            functools.partial(step_kernel, step == 0, 0.1 / (step + 1), 0.1 / max(step, 1)),
            out_shape=(sd((nf, n), F32), sd((nf, n), F32), sd((1, cols), F32), sd((8, 128), F32)),
            in_specs=[VMEM] * 8, out_specs=(VMEM,) * 4,
            scratch_shapes=[
                pltpu.VMEM((total_rows + n + ROWS, 2 * width), BF16),
                pltpu.VMEM((2 * width, cols), BF16),
                pltpu.VMEM((2, ROWS, block), F32),
                pltpu.VMEM((total_rows + n + ROWS, 128), F32),
                pltpu.VMEM((8, cols), F32),
                pltpu.VMEM((8, cols), F32),
            ],
            compiler_params=params(), name="step",
        )(facs, infos, mu, load, cust_t, hq, lam, wt)
        mus.append(mu)
        tots.append(tot[0, 0])
        payload = part
        if step == ITERS - 1:
            opened = open_flags.astype(F32)
            shut = cap_mult
            extras = []
            for k in range(ITERS):
                fixed = jnp.sum(opened * fixed_cost - (1.0 - opened) * shut * capacity)
                mine = jnp.sum(mus[k] * jnp.where(lax.broadcasted_iota(jnp.int32, (nf, n), 0) == f, infos[:, 3, :], 0.0))
                extras.append(tots[k] + jnp.where(c == 0, fixed - mine, 0.0))
                shut = jnp.maximum(0.0, shut - 0.1 / (k + 1))
            row = jnp.concatenate([jnp.stack(extras), jnp.zeros((n - ITERS,), F32)])
            payload = jnp.concatenate([part, row[None], jnp.zeros((7, n), F32)], axis=0)
        rows = payload.shape[0]
        load = pl.pallas_call(
            functools.partial(reduce_kernel, nf, nc),
            out_shape=sd((rows, n), F32), in_specs=[VMEM], out_specs=VMEM,
            scratch_shapes=[pltpu.VMEM((nc - 1, rows, n), F32), pltpu.VMEM((rows, n), F32), pltpu.VMEM((nf - 1, rows, n), F32),
                            dma((nc - 1,)), dma((nc - 1,)), dma((nf - 1,)), dma((nf - 1,))],
            compiler_params=params(1 + step), name="reduce",
        )(payload)
    lam_all = pl.pallas_call(
        functools.partial(gather_lam_kernel, nf),
        out_shape=sd((nf, 1, cols), F32), in_specs=[VMEM], out_specs=VMEM,
        scratch_shapes=[dma((nf - 1,)), dma((nf - 1,)), dma(())],
        compiler_params=params(1 + ITERS), name="lams",
    )(lam)
    bounds = load[nf, 0:ITERS] / total_cust
    total = lax.dynamic_slice_in_dim(load, f, 1, 0)
    cap = lax.dynamic_slice_in_dim(infos, f, 1, 0)[0, 3:4]
    last = lax.dynamic_slice_in_dim(mu, f, 1, 0)

    def finish(total_ref, last_ref, cap_ref, open_ref, shut_ref, out_ref):
        load, cap = total_ref[...], cap_ref[...]
        new = jnp.maximum(0.0, last_ref[...] + (0.1 / ITERS) * (load - cap) / (load + jnp.where(cap > 0, cap, 1.0)))
        hot = onehot_of(open_ref[...])
        rows = jnp.concatenate([v.astype(F32) for v in split3(new)] + [jnp.zeros((13, n), F32)], axis=0).astype(BF16)
        got = jnp.dot(rows, hot, preferred_element_type=F32)
        out_ref[...] = jnp.where(open_ref[...] > 0, got[0:1] + got[1:2] + got[2:3], shut_ref[...])

    cap_final = pl.pallas_call(finish, out_shape=sd((1, n), F32), in_specs=[VMEM] * 5, out_specs=VMEM, compiler_params=params(), name="finish")(
        total, last, cap, open_row, shut.reshape(1, n))
    return lam_all.reshape(nf * cols), cap_final.reshape(n), bounds


def solution(mesh):
    nf, nc = mesh.shape["fac"], mesh.shape["cust"]
    return jax.shard_map(
        functools.partial(local, nf, nc),
        mesh=mesh,
        in_specs=(P("fac", None), P(("cust", "fac"), None), P("fac"), P("cust"), P("fac"), P("fac"), P("fac"), P("cust")),
        out_specs=(P("cust"), P("fac"), P()),
        check_vma=False,
    )
```

```python
import functools
import math

import jax
import jax.numpy as jnp
from jax import lax
from jax.experimental import pallas as pl
from jax.experimental.pallas import tpu as pltpu
from jax.sharding import PartitionSpec as P

MESH = pl.DeviceIdType.MESH
ITERS = 3
TAU = 0.1
ALIGN = 16
ROWS = 256
F32 = jnp.float32
BF16 = jnp.bfloat16
VMEM = pl.BlockSpec(memory_space=pltpu.VMEM)


def split3(v):
    a = v.astype(BF16)
    r = v - a.astype(F32)
    b = r.astype(BF16)
    c = (r - b.astype(F32)).astype(BF16)
    return a, b, c


def onehot_of(open_row):
    n = open_row.shape[1]
    flags = jnp.broadcast_to(open_row.astype(F32), (16, n)).astype(BF16)
    tri = (lax.broadcasted_iota(jnp.int32, (n, n), 0) <= lax.broadcasted_iota(jnp.int32, (n, n), 1)).astype(F32).astype(BF16)
    pos = jnp.dot(flags, tri, preferred_element_type=F32)[0:1]
    pos = jnp.where(open_row > 0, pos - 1.0, -1.0).astype(jnp.int32)
    hit = lax.broadcasted_iota(jnp.int32, (n, n), 0) == pos
    return jnp.where(hit, 1.0, 0.0).astype(BF16)


def nt(a, b):
    return lax.dot_general(a, b, (((1,), (1,)), ((), ())), preferred_element_type=F32)


def pre_kernel(open_ref, fac_ref, cap_ref, mu_ref, fixed_ref, cust_ref, demand_ref, cover_ref,
               comp_ref, info_ref, cust_t_ref, hq_ref, wt_ref, lam_ref, ext_ref, shut_ref):
    n, width = fac_ref.shape
    cols = cust_ref.shape[0]
    nc, _, part = info_ref.shape
    f, c = lax.axis_index("fac"), lax.axis_index("cust")
    mine = pl.ds(pl.multiple_of(f * cols, cols), cols)
    wt_ref[...] = demand_ref[:, mine].astype(F32)
    lam_ref[...] = cover_ref[:, mine]
    opened = open_ref[...].astype(F32)
    shut = mu_ref[...]
    ext = jnp.zeros((8, 128), F32)
    lane = lax.broadcasted_iota(jnp.int32, (8, 128), 1)
    for k in range(ITERS):
        fixed = jnp.sum(opened * fixed_ref[...] - (1.0 - opened) * shut * cap_ref[...])
        ext = ext + jnp.where((lane == k) & (c == 0), fixed, 0.0)
        shut = jnp.maximum(0.0, shut - 0.1 / (k + 1))
    ext_ref[...] = ext
    shut_ref[...] = shut
    hot = onehot_of(open_ref[...])
    fac = fac_ref[...]
    comp_ref[...] = jnp.dot(hot, fac, preferred_element_type=F32).astype(BF16)
    sq = fac.astype(F32) ** 2
    s1, s2, _ = split3(sq)
    ones = jnp.ones((16, width), BF16)
    half = -0.5 * (nt(ones, s1) + nt(ones, s2))[0:1]
    rows = [jnp.ones((1, n), BF16)]
    for v in (half, mu_ref[...], cap_ref[...]):
        rows.extend(split3(v))
    rows = [r.astype(F32) for r in rows] + [jnp.zeros((6, n), F32)]
    got = nt(jnp.concatenate(rows, axis=0).astype(BF16), hot)
    rows = [got[0:1]] + [got[3 * m + 1:3 * m + 2] + got[3 * m + 2:3 * m + 3] + got[3 * m + 3:3 * m + 4] for m in range(3)]
    info = jnp.concatenate(rows + [jnp.zeros((4, n), F32)], axis=0)
    for p in range(nc):
        info_ref[p] = info[:, p * part:(p + 1) * part]
    eye = (lax.broadcasted_iota(jnp.int32, (width, width), 0) == lax.broadcasted_iota(jnp.int32, (width, width), 1)).astype(F32).astype(BF16)
    turned = nt(eye, cust_ref[...])
    cust_t_ref[...] = turned.astype(BF16)
    hq_ref[...] = 0.5 * jnp.sum(turned * turned, axis=0, keepdims=True)


def sync(peers):
    barrier = pltpu.get_barrier_semaphore()
    for peer in peers:
        pl.semaphore_signal(barrier, inc=1, device_id=peer, device_id_type=MESH)
    pl.semaphore_wait(barrier, len(peers))


def gather_kernel(nf, nc, comp_ref, info_ref, facs_ref, infos_ref, s1, r1, s2, r2, s3, r3, loc):
    f, c = lax.axis_index("fac"), lax.axis_index("cust")
    fp = [(lax.rem(f + d, nf), c) for d in range(1, nf)]
    half = nc // 2
    core = lax.rem(c, 2)
    twin = (f, c + 1 - 2 * core)
    sides = [lax.rem(c + 2 * d, nc) for d in range(1, half)]
    part = comp_ref.shape[0] // nc
    sync(fp + [(f, e) for e in sides] + [twin])

    def rows(q):
        return pl.ds(pl.multiple_of(q * part, part), part)

    def move(src, q, k, send, recv, peer, own=False):
        a = comp_ref.at[rows(q)] if own else facs_ref.at[src, rows(q)]
        b = info_ref.at[q] if own else infos_ref.at[src, q]
        pair = [
            pltpu.make_async_remote_copy(a, facs_ref.at[src, rows(q)], send.at[k, 0], recv.at[k, 0], device_id=peer, device_id_type=MESH),
            pltpu.make_async_remote_copy(b, infos_ref.at[src, q], send.at[k, 1], recv.at[k, 1], device_id=peer, device_id_type=MESH),
        ]
        for cpy in pair:
            cpy.start()
        return pair

    first = [move(f, c, d, s1, r1, peer, True) for d, peer in enumerate(fp)]
    own = pltpu.make_async_copy(comp_ref, facs_ref.at[f], loc.at[0])
    own.start()
    own_info = pltpu.make_async_copy(info_ref, infos_ref.at[f], loc.at[1])
    own_info.start()
    across, over = [], []
    for d in range(nf - 1):
        src = lax.rem(f + nf - 1 - d, nf)
        for cpy in first[d]:
            cpy.wait_recv()
        for e, q in enumerate(sides):
            across.append((src, lax.rem(c + nc - 2 * (e + 1), nc), move(src, c, d * (half - 1) + e, s2, r2, (f, q))))
        over.append(move(src, c, d * half, s3, r3, twin))
        for e in range(half - 1):
            if d > 0:
                ready = across[(d - 1) * (half - 1) + e]
                for cpy in ready[2]:
                    cpy.wait_recv()
                over.append(move(ready[0], ready[1], (d - 1) * half + 1 + e, s3, r3, twin))
    for e in range(half - 1):
        ready = across[(nf - 2) * (half - 1) + e]
        for cpy in ready[2]:
            cpy.wait_recv()
        over.append(move(ready[0], ready[1], (nf - 2) * half + 1 + e, s3, r3, twin))
    for pair in first + [a[2] for a in across]:
        for cpy in pair:
            cpy.wait_send()
    for pair in over:
        for cpy in pair:
            cpy.wait()
    own.wait()
    own_info.wait()


def step_kernel(step, facs_ref, infos_ref, mu_ref, load_ref, cust_t_ref, hq_ref, lam_ref, wt_ref, ext_ref,
                part_ref, mu_out_ref, lam_out_ref, tot_ref,
                info_ref, a_ref, w_ref, y_ref, x_ref, d_ref, acc_ref, cov_ref, soft_ref):
    first, size, prev = step == 0, 0.1 / (step + 1), 0.1 / max(step, 1)
    nf, n, width = facs_ref.shape
    cols = cust_t_ref.shape[1]
    block = y_ref.shape[2]
    tiles = cols // block
    lam = lam_ref[...]
    wt = wt_ref[...]
    a1, a2, a3 = split3(64.0 * lam - hq_ref[...])
    one_c = jnp.ones((3, cols), F32)
    mw = jnp.broadcast_to(-64.0 * wt, (3, cols))
    aug = jnp.concatenate([a1.astype(F32), a2.astype(F32), a3.astype(F32), one_c, mw, jnp.zeros((7, cols), F32)], axis=0)
    w_ref[0:width, :] = cust_t_ref[...]
    w_ref[width:width + 16, :] = aug.astype(BF16)
    w_ref[width + 16:, :] = jnp.zeros((width - 16, cols), BF16)
    cov_ref[...] = jnp.zeros_like(cov_ref)
    soft_ref[...] = jnp.zeros_like(soft_ref)
    lane = lax.broadcasted_iota(jnp.int32, (ROWS, width), 1)
    pad = jnp.where(lane == 3, -30000.0, 0.0).astype(BF16)
    sel = (lax.broadcasted_iota(jnp.int32, (16, width), 0) == lax.broadcasted_iota(jnp.int32, (16, width), 1)).astype(F32).astype(BF16)
    top = (lax.broadcasted_iota(jnp.int32, (16, 128), 0) == 0).astype(F32).astype(BF16)
    wrows = jnp.concatenate([wt, jnp.zeros((15, cols), F32)], axis=0).astype(BF16)
    d_ref[...] = lax.dot_general(wrows, top, (((0,), (0,)), ((), ())), preferred_element_type=F32).astype(BF16)
    nc, part = infos_ref.shape[1], infos_ref.shape[3]
    for f in range(nf):
        info_ref[f] = jnp.concatenate([infos_ref[f, p] for p in range(nc)], axis=1)
    offs = []
    off = jnp.int32(0)
    one_r = jnp.ones((3, n), F32)
    for f in range(nf):
        valid = info_ref[f, 0:1, :]
        cap = info_ref[f, 3:4, :]
        if first:
            mu = info_ref[f, 2:3, :]
        else:
            mu = mu_ref[f:f + 1, :]
            load = load_ref[f:f + 1, :]
            mu = jnp.maximum(0.0, mu + prev * (load - cap) / (load + jnp.where(valid > 0, cap, 1.0)))
        mu = mu * valid
        mu_out_ref[f:f + 1, :] = mu
        b = jnp.where(valid > 0, info_ref[f, 1:2, :], -30000.0)
        parts = [p.astype(F32) for p in split3(b) + split3(mu)]
        rows = jnp.concatenate([one_r] + parts + [jnp.zeros((7, n), F32)], axis=0).astype(BF16)
        side = lax.dot_general(rows, sel, (((0,), (0,)), ((), ())), preferred_element_type=F32).astype(BF16)
        count = jnp.sum(valid).astype(jnp.int32)
        off = pl.multiple_of(off, ALIGN)
        offs.append(off)
        a_ref[pl.ds(off, n), 0:width] = facs_ref[f]
        a_ref[pl.ds(off, n), width:2 * width] = side
        off = off + ((count + ALIGN - 1) // ALIGN) * ALIGN
    tail = pl.multiple_of(off, ALIGN)
    a_ref[pl.ds(tail, ROWS), 0:width] = jnp.zeros((ROWS, width), BF16)
    a_ref[pl.ds(tail, ROWS), width:2 * width] = pad
    n_blocks = (off + ROWS - 1) // ROWS
    scale = math.log2(math.e) / 6.4

    def body(i, _):
        base = pl.multiple_of(i * ROWS, ROWS)
        lhs = a_ref[pl.ds(base, ROWS), :]

        def dot(t):
            y_ref[t % 2] = jnp.dot(lhs, w_ref[:, t * block:(t + 1) * block], preferred_element_type=F32)

        dot(0)
        for t in range(tiles):
            if t + 1 < tiles:
                dot(t + 1)
            covs = [cov_ref[:, t * block + q * 128:t * block + (q + 1) * 128] for q in range(block // 128)]
            softs = [soft_ref[:, t * block + q * 128:t * block + (q + 1) * 128] for q in range(block // 128)]
            for r in range(0, ROWS, 32):
                for q in range(block // 128):
                    es = [jnp.exp2(y_ref[t % 2, r + 8 * s:r + 8 * s + 8, q * 128:(q + 1) * 128] * scale) for s in range(4)]
                    us = [1.0 + e for e in es]
                    p01 = us[0] * us[1]
                    p23 = us[2] * us[3]
                    r01 = 1.0 / p01
                    r23 = 1.0 / p23
                    xs = [es[0] * (us[1] * r01), es[1] * (us[0] * r01), es[2] * (us[3] * r23), es[3] * (us[2] * r23)]
                    covs[q] = covs[q] + ((xs[0] + xs[1]) + (xs[2] + xs[3]))
                    softs[q] = softs[q] + jnp.log(p01 * p23)
                    for h in range(2):
                        both = jnp.concatenate([xs[2 * h], xs[2 * h + 1]], axis=0).astype(BF16)
                        x_ref[t % 2, r + 16 * h:r + 16 * h + 16, q * 128:(q + 1) * 128] = both
            got = jnp.dot(x_ref[t % 2], d_ref[t * block:(t + 1) * block, :], preferred_element_type=F32)
            at = pl.ds(base, ROWS)
            acc_ref[at, :] = got if t == 0 else acc_ref[at, :] + got
            for q in range(block // 128):
                cov_ref[:, t * block + q * 128:t * block + (q + 1) * 128] = covs[q]
                soft_ref[:, t * block + q * 128:t * block + (q + 1) * 128] = softs[q]
        return 0

    lax.fori_loop(0, n_blocks, body, 0)
    diag = lax.broadcasted_iota(jnp.int32, (128, 128), 0) == lax.broadcasted_iota(jnp.int32, (128, 128), 1)
    for f in range(nf):
        for b in range(n // 128):
            at = pl.ds(pl.multiple_of(offs[f] + b * 128, ALIGN), 128)
            got = jnp.sum(jnp.where(diag, acc_ref[at, :], 0.0), axis=0, keepdims=True)
            part_ref[f:f + 1, b * 128:(b + 1) * 128] = jnp.where(info_ref[f, 0:1, b * 128:(b + 1) * 128] > 0, got, 0.0)
    cover = jnp.sum(cov_ref[...], axis=0, keepdims=True)
    soft = jnp.sum(soft_ref[...], axis=0, keepdims=True)
    me, c = lax.axis_index("fac"), lax.axis_index("cust")
    mine = jnp.sum(mu_out_ref[pl.ds(me, 1), :] * info_ref[me, 3:4, :])
    here = jnp.sum(wt * lam - TAU * wt * soft) - jnp.where(c == 0, mine, 0.0)
    spot = lax.broadcasted_iota(jnp.int32, (8, 128), 1) == step
    tot = ext_ref[...] + jnp.where(spot, here, 0.0)
    tot_ref[...] = tot
    if part_ref.shape[0] > nf:
        part_ref[nf:nf + 8, :] = jnp.zeros((8, n), F32)
        part_ref[nf:nf + 8, 0:128] = tot
    lam_out_ref[...] = lam + size * wt * (1.0 - cover) / (1.0 + cover)


def exchange(peers, src, slots, send, recv):
    copies = []
    for d, peer in enumerate(peers):
        cpy = pltpu.make_async_remote_copy(src, slots.at[d], send.at[d], recv.at[d], device_id=peer, device_id_type=MESH)
        cpy.start()
        copies.append(cpy)
    return copies


def reduce_kernel(nf, nc, x_ref, lam_ref, out_ref, lam_out, got1, mid, got2, s1, r1, s2, r2, s3, r3, loc):
    f, c = lax.axis_index("fac"), lax.axis_index("cust")
    fp = [(lax.rem(f + d, nf), c) for d in range(1, nf)]
    cp = [(f, lax.rem(c + d, nc)) for d in range(1, nc)]
    sync(fp + cp)
    first = exchange(cp, x_ref, got1, s1, r1)
    lams = []
    if lam_ref is not None:
        own = pltpu.make_async_copy(lam_ref, lam_out.at[f], loc)
        own.start()
        for d, peer in enumerate(fp):
            cpy = pltpu.make_async_remote_copy(lam_ref, lam_out.at[f], s3.at[d], r3.at[d], device_id=peer, device_id_type=MESH)
            cpy.start()
            lams.append(cpy)
    total = x_ref[...]
    for d, cpy in enumerate(first):
        cpy.wait()
        total = total + got1[d]
    mid[...] = total
    second = exchange(fp, mid, got2, s2, r2)
    for d, cpy in enumerate(second):
        cpy.wait()
        total = total + got2[d]
    out_ref[...] = total
    for cpy in lams:
        cpy.wait()
    if lam_ref is not None:
        own.wait()


def reduce_plain(nf, nc, x_ref, out_ref, got1, mid, got2, s1, r1, s2, r2):
    reduce_kernel(nf, nc, x_ref, None, out_ref, None, got1, mid, got2, s1, r1, s2, r2, None, None, None)


def finish_kernel(total_cust, total_ref, mu_ref, infos_ref, open_ref, shut_ref, out_ref, bound_ref):
    nf, nc = infos_ref.shape[0:2]
    n = open_ref.shape[1]
    f = lax.axis_index("fac")
    load = total_ref[pl.ds(f, 1), :]
    cap = jnp.concatenate([infos_ref[f, p, 3:4, :] for p in range(nc)], axis=1)
    new = jnp.maximum(0.0, mu_ref[pl.ds(f, 1), :] + (0.1 / ITERS) * (load - cap) / (load + jnp.where(cap > 0, cap, 1.0)))
    rows = jnp.concatenate([v.astype(F32) for v in split3(new)] + [jnp.zeros((13, n), F32)], axis=0).astype(BF16)
    got = jnp.dot(rows, onehot_of(open_ref[...]), preferred_element_type=F32)
    out_ref[...] = jnp.where(open_ref[...] > 0, got[0:1] + got[1:2] + got[2:3], shut_ref[...])
    bound_ref[...] = total_ref[nf:nf + 1, 0:128] / total_cust


def params(cid=None, mib=56):
    return pltpu.CompilerParams(collective_id=cid, has_side_effects=True, vmem_limit_bytes=mib * 2 ** 20) if cid is not None else pltpu.CompilerParams(vmem_limit_bytes=mib * 2 ** 20)


def local(nf, nc, fac_coords, cust_coords, open_flags, demand, fixed_cost, capacity, cap_mult, cover_mult):
    n, width = fac_coords.shape
    cols = cust_coords.shape[0]
    total_cust = cols * nf * nc
    sd = jax.ShapeDtypeStruct
    dma = pltpu.SemaphoreType.DMA
    part = n // nc
    open_row = open_flags.reshape(1, n)
    comp, info, cust_t, hq, wt, lam, ext, shut = pl.pallas_call(
        pre_kernel,
        out_shape=(sd((n, width), BF16), sd((nc, 8, part), F32), sd((width, cols), BF16), sd((1, cols), F32),
                   sd((1, cols), F32), sd((1, cols), F32), sd((8, 128), F32), sd((1, n), F32)),
        in_specs=[VMEM] * 8, out_specs=(VMEM,) * 8, compiler_params=params(), name="pre",
    )(open_row, fac_coords, capacity.reshape(1, n), cap_mult.reshape(1, n), fixed_cost.reshape(1, n), cust_coords,
      demand.reshape(1, nf * cols), cover_mult.reshape(1, nf * cols))
    sides = (nf - 1) * (nc // 2 - 1)
    facs, infos = pl.pallas_call(
        functools.partial(gather_kernel, nf, nc),
        out_shape=(sd((nf, n, width), BF16), sd((nf, nc, 8, part), F32)),
        in_specs=[VMEM] * 2, out_specs=(VMEM,) * 2,
        scratch_shapes=[dma((nf - 1, 2)), dma((nf - 1, 2)), dma((sides, 2)), dma((sides, 2)),
                        dma(((nf - 1) * (nc // 2), 2)), dma(((nf - 1) * (nc // 2), 2)), dma((2,))],
        compiler_params=params(0), name="gather",
    )(comp, info)
    block = math.gcd(cols, 512)
    total_rows = nf * n
    mu = load = hq
    tot = ext
    for step in range(ITERS):
        last = step == ITERS - 1
        rows = nf + 8 if last else nf
        payload, mu, lam, tot = pl.pallas_call(
            functools.partial(step_kernel, step),
            out_shape=(sd((rows, n), F32), sd((nf, n), F32), sd((1, cols), F32), sd((8, 128), F32)),
            in_specs=[VMEM] * 9, out_specs=(VMEM,) * 4,
            scratch_shapes=[
                pltpu.VMEM((nf, 8, n), F32),
                pltpu.VMEM((total_rows + n + ROWS, 2 * width), BF16),
                pltpu.VMEM((2 * width, cols), BF16),
                pltpu.VMEM((2, ROWS, block), F32),
                pltpu.VMEM((2, ROWS, block), BF16),
                pltpu.VMEM((cols, 128), BF16),
                pltpu.VMEM((total_rows + n + ROWS, 128), F32),
                pltpu.VMEM((8, cols), F32),
                pltpu.VMEM((8, cols), F32),
            ],
            compiler_params=params(), name="step",
        )(facs, infos, mu, load, cust_t, hq, lam, wt, tot)
        scratch = [pltpu.VMEM((nc - 1, rows, n), F32), pltpu.VMEM((rows, n), F32), pltpu.VMEM((nf - 1, rows, n), F32),
                   dma((nc - 1,)), dma((nc - 1,)), dma((nf - 1,)), dma((nf - 1,))]
        if not last:
            load = pl.pallas_call(
                functools.partial(reduce_plain, nf, nc),
                out_shape=sd((rows, n), F32), in_specs=[VMEM], out_specs=VMEM,
                scratch_shapes=scratch, compiler_params=params(1 + step), name="reduce",
            )(payload)
        else:
            load, lam_all = pl.pallas_call(
                functools.partial(reduce_kernel, nf, nc),
                out_shape=(sd((rows, n), F32), sd((nf, 1, cols), F32)), in_specs=[VMEM] * 2, out_specs=(VMEM,) * 2,
                scratch_shapes=scratch + [dma((nf - 1,)), dma((nf - 1,)), dma(())],
                compiler_params=params(1 + step), name="reduce",
            )(payload, lam)
    cap_final, bounds = pl.pallas_call(
        functools.partial(finish_kernel, total_cust), out_shape=(sd((1, n), F32), sd((1, 128), F32)),
        in_specs=[VMEM] * 5, out_specs=(VMEM,) * 2, compiler_params=params(), name="finish",
    )(load, mu, infos, open_row, shut)
    return lam_all.reshape(nf * cols), cap_final.reshape(n), bounds[0, :ITERS]


def solution(mesh):
    nf, nc = mesh.shape["fac"], mesh.shape["cust"]
    return jax.shard_map(
        functools.partial(local, nf, nc),
        mesh=mesh,
        in_specs=(P("fac", None), P(("cust", "fac"), None), P("fac"), P("cust"), P("fac"), P("fac"), P("fac"), P("cust")),
        out_specs=(P("cust"), P("fac"), P()),
        check_vma=False,
    )
```
